768 devices in a mesh: shard: 24 (over y, z_lo), replica: 32 (over z_hi, x, core).
Axes of the slice: x: 4, y: 8, z: 12 (z_hi: 4, z_lo: 3; z = z_hi * 3 + z_lo), core: 2. Of those that a mesh axis runs over, the one named last changes fastest.
Arguments:
- scan_input: bfloat16 [147456, 1024], P(('shard', 'replica')), may hold values from -6 to 6
- gate_input: bfloat16 [147456, 1024], P(('shard', 'replica')), may hold values from -6 to 6
- write_proj: bfloat16 [147456, 128], P(('shard', 'replica')), may hold values from -2 to 2
- read_proj: bfloat16 [147456, 128], P(('shard', 'replica')), may hold values from -2 to 2
- step_raw: float32 [16, 147456], P(None, ('shard', 'replica')), may hold values from -4 to 4
- decay_log: float32 [16], replicated, may hold values from 0 to 2.5
- step_bias: float32 [16], replicated, may hold values from -6 to -2.5
- skip_gain: float32 [16], replicated, may hold values from 0.5 to 1.5
- norm_gain: float32 [1024], replicated, may hold values from 0.25 to 1.75
- out_weight: bfloat16 [1024, 2304], P('replica'), may hold values from -0.1875 to 0.1875
- out_grad: bfloat16 [147456, 2304], P(('shard', 'replica')), may hold values from -6 to 6
Outputs:
- grad_weight: float32 [1024, 2304], P('replica')
- grad_input: bfloat16 [147456, 1024], P(('shard', 'replica'))
- grad_gate: bfloat16 [147456, 1024], P(('shard', 'replica'))
- grad_write: bfloat16 [147456, 128], P(('shard', 'replica'))
- grad_read: bfloat16 [147456, 128], P(('shard', 'replica'))
- grad_step: float32 [16, 147456], P(None, ('shard', 'replica'))
- grad_decay: float32 [16], replicated
- grad_bias: float32 [16], replicated
- grad_skip: float32 [16], replicated
- grad_gain: float32 [1024], replicated
The draws below stay inside these ranges and needn't reach their ends.
All inputs are finite; a program needn't handle non-finite values.
Results may differ from the reference program's by a relative error of at most 0.024.
Values may be sent and summed in bfloat16 or wider, within the bound.
No kernel may reach another device: no remote copies, remote signals or barrier semaphores. Data moves between devices by JAX's collectives and lax.ppermute only.
A program may use at most 64 MiB of HBM per device.

```python
import jax
import jax.numpy as jnp
from jax import lax

COLS = 2304
P_SIZE = 64
N = 128
H = 16
TOK_DEV = 192
TOKENS = 147456


def steps_of(key, extent, cuts, low, high):
    gain, own = 1.0, jax.random.fold_in(key, 6)
    for position, blocks in cuts:
        steps = jnp.exp(jax.random.uniform(jax.random.fold_in(own, position), (blocks,), jnp.float32, low / len(cuts), high / len(cuts)))
        gain = gain * jnp.repeat(steps, extent[position] // blocks).reshape([-1 if axis == position else 1 for axis in range(len(extent))])
    return gain


def bell_draw(stream_key, extent, width, bound, cuts=(), kind=jnp.bfloat16):
    gain = steps_of(stream_key, extent, cuts, -0.22, 0.18) if cuts else 1.0
    entries = jax.random.normal(stream_key, extent, jnp.float32) * width * gain
    return jnp.minimum(jnp.maximum(entries, -bound), bound).astype(kind)


def setup_inputs(seed: int = 0) -> dict:
    streams_of = jax.random.split(jax.random.key(seed), 12)
    scan_input = bell_draw(streams_of[0], (TOKENS, H * P_SIZE), 1.0, 6.0, ((0, 768),))
    gate_input = bell_draw(streams_of[1], (TOKENS, H * P_SIZE), 1.0, 6.0, ((0, 768),))
    write_proj = bell_draw(streams_of[2], (TOKENS, N), 0.3, 2.0, ((0, 768),))
    read_proj = bell_draw(streams_of[3], (TOKENS, N), 0.3, 2.0, ((0, 768),))
    step_raw = bell_draw(streams_of[4], (H, TOKENS), 1.0, 4.0, ((1, 768),), jnp.float32)
    decay_log = jnp.clip(jax.random.uniform(streams_of[5], (H,), jnp.float32, 0.0, 2.5), 0.0, 2.5)
    step_bias = jnp.clip(jax.random.uniform(streams_of[6], (H,), jnp.float32, -6.0, -2.5), -6.0, -2.5)
    skip_gain = jnp.clip(jax.random.uniform(streams_of[7], (H,), jnp.float32, 0.5, 1.5), 0.5, 1.5)
    norm_gain = jnp.clip(1.0 + 0.15 * jax.random.normal(streams_of[8], (H * P_SIZE,), jnp.float32), 0.25, 1.75)
    out_weight = bell_draw(streams_of[9], (H * P_SIZE, COLS), (H * P_SIZE) ** -0.5, 0.1875, ((0, 32),))
    out_grad = bell_draw(streams_of[10], (TOKENS, COLS), 1.0, 6.0, ((0, 768),))
    return dict(scan_input=scan_input, gate_input=gate_input, write_proj=write_proj, read_proj=read_proj, step_raw=step_raw, decay_log=decay_log, step_bias=step_bias, skip_gain=skip_gain, norm_gain=norm_gain, out_weight=out_weight, out_grad=out_grad)


def forward(scan_input, gate_input, write_proj, read_proj, step_raw, decay_log, step_bias, skip_gain, norm_gain):
    length = scan_input.shape[0]
    head_count = step_raw.shape[0]
    inputs = scan_input.astype(jnp.float32).reshape(length, head_count, -1)
    step_size = jax.nn.softplus(step_raw + step_bias[:, None])
    decay_rate = -jnp.exp(decay_log)
    cumulative = jnp.cumsum(step_size * decay_rate[:, None], axis=1)
    positions = jnp.arange(length, dtype=jnp.int32)
    causal = positions[:, None] >= positions[None, :]
    log_decay = jnp.where(causal[None], cumulative[:, :, None] - cumulative[:, None, :], 0.0)
    decay_mask = jnp.where(causal[None], jnp.exp(log_decay), 0.0)
    scores = jnp.dot(read_proj, write_proj.T, preferred_element_type=jnp.float32)
    weights = decay_mask * scores[None] * step_size[:, None, :]
    mixed = jnp.einsum('hts,shp->thp', weights, inputs, precision=lax.Precision.HIGHEST)
    mixed = mixed + skip_gain[None, :, None] * inputs
    gated = mixed.reshape(length, -1) * jax.nn.silu(gate_input.astype(jnp.float32))
    inverse_rms = lax.rsqrt(lax.optimization_barrier(jnp.mean(gated * gated, axis=1, keepdims=True)) + 1e-05)
    return gated * inverse_rms * norm_gain[None, :]

def reference(scan_input, gate_input, write_proj, read_proj, step_raw, decay_log, step_bias, skip_gain, norm_gain, out_weight, out_grad):
    channels = scan_input.shape[1]
    head_count = step_raw.shape[0]
    seq_count = scan_input.shape[0] // TOK_DEV

    def by_sequence(values):
        return values.reshape(seq_count, TOK_DEV, values.shape[1])
    raw_steps = step_raw.reshape(head_count, seq_count, TOK_DEV).transpose(1, 0, 2)

    def per_sequence(total, packed):
        inputs, gates, writes, reads, raw_part, grad_part = packed
        cotangent = jnp.dot(grad_part, out_weight.T, preferred_element_type=jnp.float32)
        normed, pull_back = jax.vjp(forward, inputs, gates, writes, reads, raw_part, decay_log, step_bias, skip_gain, norm_gain)
        normed_half = normed.astype(jnp.bfloat16)
        term = jnp.dot(normed_half.T, grad_part, preferred_element_type=jnp.float32).astype(jnp.bfloat16)
        term = lax.optimization_barrier(term)
        return (total + term.astype(jnp.float32), pull_back(cotangent))
    start = jnp.zeros((channels, out_grad.shape[1]), jnp.float32)
    grad_weight, gradients = lax.scan(per_sequence, start, (by_sequence(scan_input), by_sequence(gate_input), by_sequence(write_proj), by_sequence(read_proj), raw_steps, by_sequence(out_grad)))
    grad_input = gradients[0].reshape(-1, channels)
    grad_gate = gradients[1].reshape(-1, channels)
    grad_write = gradients[2].reshape(-1, write_proj.shape[1])
    grad_read = gradients[3].reshape(-1, read_proj.shape[1])
    grad_step = gradients[4].transpose(1, 0, 2).reshape(head_count, -1)
    grad_decay = lax.optimization_barrier(jnp.sum(gradients[5], axis=0))
    grad_bias = lax.optimization_barrier(jnp.sum(gradients[6], axis=0))
    grad_skip = lax.optimization_barrier(jnp.sum(gradients[7], axis=0))
    grad_gain = lax.optimization_barrier(jnp.sum(gradients[8], axis=0))
    return (grad_weight, grad_input, grad_gate, grad_write, grad_read, grad_step, grad_decay, grad_bias, grad_skip, grad_gain)
```

```python
import functools

import jax
import jax.numpy as jnp
from jax import lax
from jax.sharding import Mesh
from jax.sharding import PartitionSpec as P

AXES = ("y", "zl", "zh", "xa", "xb", "c")
REPLICA = ("zh", "xa", "xb", "c")
NODE_X = ("xa", "xb")
NODE = ("xa", "xb", "c")
LINE = ("zl", "zh")
SWAP = [(0, 1), (1, 0)]


def shift(devices, by):
    return [(i, (i + by) % devices) for i in range(devices)]


def along_line(by):
    place = [(z % 3) * 4 + z // 3 for z in range(12)]
    return [(place[z], place[(z + by) % 12]) for z in range(12)]


def in_order(parts, first):
    count = len(parts)
    return lax.dynamic_slice_in_dim(jnp.stack(parts * 2), (count - first) % count, count, 0)


def part_of(value, index):
    return lax.dynamic_index_in_dim(value, index, 0, keepdims=False)


def exchange(tiles, axes):
    return lax.all_to_all(tiles, axes, 0, 0, tiled=True)


def forward(
    scan_input,
    gate_input,
    write_proj,
    read_proj,
    step_raw,
    decay_log,
    step_bias,
    skip_gain,
    norm_gain,
):
    length = scan_input.shape[0]
    head_count = step_raw.shape[0]
    inputs = scan_input.astype(jnp.float32).reshape(length, head_count, -1)
    step_size = jax.nn.softplus(step_raw + step_bias[:, None])
    decay_rate = -jnp.exp(decay_log)
    cumulative = jnp.cumsum(step_size * decay_rate[:, None], axis=1)
    positions = jnp.arange(length, dtype=jnp.int32)
    causal = positions[:, None] >= positions[None, :]
    log_decay = jnp.where(causal[None], cumulative[:, :, None] - cumulative[:, None, :], 0.0)
    decay_mask = jnp.where(causal[None], jnp.exp(log_decay), 0.0)
    scores = jnp.dot(read_proj, write_proj.T, preferred_element_type=jnp.float32)
    weights = decay_mask * scores[None] * step_size[:, None, :]
    mixed = jnp.einsum("hts,shp->thp", weights, inputs, precision=lax.Precision.HIGHEST)
    mixed = mixed + skip_gain[None, :, None] * inputs
    gated = mixed.reshape(length, -1) * jax.nn.silu(gate_input.astype(jnp.float32))
    inverse_rms = lax.rsqrt(jnp.mean(gated * gated, axis=1, keepdims=True) + 1e-05)
    return gated * inverse_rms * norm_gain[None, :]


def dot(left, right, dims):
    return lax.dot_general(left, right, (dims, ((), ())), preferred_element_type=jnp.float32)


def shards(
    scan_input,
    gate_input,
    write_proj,
    read_proj,
    step_raw,
    decay_log,
    step_bias,
    skip_gain,
    norm_gain,
    out_weight,
    out_grad,
):
    tokens, cols = out_grad.shape
    own_rows = out_weight.shape[0]
    half, third = cols // 2, cols // 6
    x_b, core, z_lo, z_hi = (lax.axis_index(n) for n in ("xb", "c", "zl", "zh"))

    halves = out_grad.reshape(tokens, 2, half).transpose(1, 0, 2)
    grad_near = exchange(jnp.concatenate([halves, halves]), NODE_X)
    grad_far = lax.ppermute(grad_near, "c", SWAP)

    w_halves = out_weight.reshape(own_rows, 2, half).transpose(1, 0, 2)
    w_other = lax.ppermute(part_of(w_halves, 1 - x_b), "xb", SWAP)
    w_pair = in_order([part_of(w_halves, x_b), w_other], x_b)
    w_third = part_of(w_pair.reshape(2 * own_rows, 3, third).transpose(1, 0, 2), z_lo)
    w_line = in_order([w_third] + [lax.ppermute(w_third, "zh", shift(4, -k)) for k in (1, 2, 3)], z_hi)
    w_line = w_line.reshape(8 * own_rows, third)
    w_next = lax.ppermute(w_line, LINE, along_line(-1))
    w_last = lax.ppermute(w_line, LINE, along_line(1))
    weight = in_order([w_line, w_next, w_last], z_lo).transpose(1, 0, 2).reshape(8 * own_rows, half)

    normed, pull_back = jax.vjp(
        forward,
        scan_input,
        gate_input,
        write_proj,
        read_proj,
        step_raw,
        decay_log,
        step_bias,
        skip_gain,
        norm_gain,
    )
    channels = 8 * own_rows
    sent = normed.astype(jnp.bfloat16).reshape(tokens, 4, 2, 2, 2, own_rows)
    sent = sent.transpose(2, 4, 0, 1, 3, 5).reshape(2, 1, 2, tokens, channels)
    sent = jnp.broadcast_to(sent, (2, 2, 2, tokens, channels)).reshape(8, tokens, channels)
    normed_node = exchange(sent, NODE).reshape(4, 2, tokens, channels)
    normed_near = lax.dynamic_index_in_dim(normed_node, core, 1, keepdims=False)
    normed_far = lax.dynamic_index_in_dim(normed_node, 1 - core, 1, keepdims=False)

    near = dot(grad_near.reshape(4 * tokens, half), weight, ((1,), (1,))).astype(jnp.bfloat16)
    far = dot(grad_far.reshape(4 * tokens, half), weight, ((1,), (1,))).astype(jnp.bfloat16)
    partial = in_order([near.reshape(4, tokens, channels), far.reshape(4, tokens, channels)], core)
    partial = partial.transpose(1, 0, 2, 3).reshape(8, tokens, channels)
    partial = exchange(partial, NODE).reshape(2, 2, 2, tokens, channels)
    grad_normed = partial.astype(jnp.float32).sum(1).reshape(2, 2, tokens, 4, 2, own_rows)
    grad_normed = grad_normed.transpose(2, 3, 0, 4, 1, 5).reshape(tokens, 4 * channels)
    gradients = pull_back(grad_normed)

    term = dot(normed_near.reshape(-1, channels), grad_near.reshape(-1, half), ((0,), (0,)))
    term = term + dot(normed_far.reshape(-1, channels), grad_far.reshape(-1, half), ((0,), (0,)))
    thirds = term.astype(jnp.bfloat16).reshape(channels, 3, third).transpose(1, 0, 2)
    from_last = lax.ppermute(part_of(thirds, (z_lo + 1) % 3), LINE, along_line(1))
    from_next = lax.ppermute(part_of(thirds, (z_lo + 2) % 3), LINE, along_line(-1))
    run = sum(v.astype(jnp.float32) for v in (part_of(thirds, z_lo), from_last, from_next))
    rows = own_rows // 8
    run = run.astype(jnp.bfloat16).reshape(4, 2, 8, rows, third).transpose(2, 0, 1, 3, 4)
    pieces = exchange(run.reshape(64, rows, third), ("y", "zh", "xb"))
    piece = pieces.astype(jnp.float32).reshape(32, 2, rows, third).sum(0)
    owned = exchange(jnp.broadcast_to(piece[None], (24, 2, rows, third)), ("y", "zl"))
    owned = owned.reshape(8, 3, 2, rows, third).transpose(0, 3, 2, 1, 4)
    grad_weight = owned.reshape(own_rows, cols)

    totals = gradients[5:9]
    for axis in ("c", NODE_X, "zh", "zl", "y"):
        totals = lax.psum(totals, axis)
    return (grad_weight, *gradients[:5], *totals)


def solution(mesh):
    torus = Mesh(mesh.devices.reshape(8, 3, 4, 2, 2, 2), AXES)
    return jax.shard_map(
        shards,
        mesh=torus,
        in_specs=(
            P(AXES, None),
            P(AXES, None),
            P(AXES, None),
            P(AXES, None),
            P(None, AXES),
            P(),
            P(),
            P(),
            P(),
            P(REPLICA, None),
            P(AXES, None),
        ),
        out_specs=(
            P(REPLICA, None),
            P(AXES, None),
            P(AXES, None),
            P(AXES, None),
            P(AXES, None),
            P(None, AXES),
            P(),
            P(),
            P(),
            P(),
        ),
        check_vma=False,
    )
```

```python
import jax
import jax.numpy as jnp
from jax import lax
from jax.experimental import pallas as pl
from jax.experimental.pallas import tpu as pltpu
from jax.sharding import Mesh
from jax.sharding import PartitionSpec as P

AXES = ("y", "zl", "zh", "xa", "xb", "c")
REPLICA = ("zh", "xa", "xb", "c")
NODE = ("xa", "xb")
LINE = ("zl", "zh")
SWAP = [(0, 1), (1, 0)]
L, D, N, H, PS = 192, 1024, 128, 16, 64
F32, BF = jnp.float32, jnp.bfloat16
VM = pl.BlockSpec(memory_space=pltpu.VMEM)
SM = pl.BlockSpec(memory_space=pltpu.SMEM)


def along_line(by):
    place = [(z % 3) * 4 + z // 3 for z in range(12)]
    return [(place[z], place[(z + by) % 12]) for z in range(12)]


def mm(a, b, ca, cb):
    return lax.dot_general(a, b, (((ca,), (cb,)), ((), ())), preferred_element_type=F32)


def split2(v):
    hi = v.astype(BF)
    return hi, (v - hi.astype(F32)).astype(BF)


def split3(v):
    hi = v.astype(BF)
    rest = v - hi.astype(F32)
    mid = rest.astype(BF)
    return hi, mid, (rest - mid.astype(F32)).astype(BF)


def column(ref):
    head = lax.broadcasted_iota(jnp.int32, (H, 128), 0)
    out = jnp.zeros((H, 128), F32)
    for h in range(H):
        out = jnp.where(head == h, ref[h], out)
    return out[:, :1]


def steps_and_decay(step_raw, decay_log, step_bias):
    step = jax.nn.softplus(step_raw + step_bias)
    rate = -jnp.exp(decay_log)
    s = lax.broadcasted_iota(jnp.int32, (L, L), 0)
    t = lax.broadcasted_iota(jnp.int32, (L, L), 1)
    upto = (s <= t).astype(BF)
    cum = sum(mm(part, upto, 1, 0) for part in split3(step * rate))
    return step, rate, cum


def causal_mask():
    t = lax.broadcasted_iota(jnp.int32, (L, L), 0)
    s = lax.broadcasted_iota(jnp.int32, (L, L), 1)
    return t >= s


def forward_kernel(dl_ref, sb_ref, skip_ref, x_ref, gate_ref, b_ref, c_ref, raw_ref, gain_ref, mixed_ref, out_ref, gated_ref):
    step, _, cum = steps_and_decay(raw_ref[...], column(dl_ref), column(sb_ref))
    cum_t = cum.T
    scores = mm(c_ref[...], b_ref[...], 1, 1)
    causal = causal_mask()
    first = lax.broadcasted_iota(jnp.int32, (L, 2 * PS), 1) < PS
    square = jnp.zeros((L, 1), F32)
    for pair in range(H // 2):
        at = slice(pair * 128, (pair + 1) * 128)
        x = x_ref[:, at]
        halves = []
        for h in (2 * pair, 2 * pair + 1):
            decay = jnp.exp(jnp.where(causal, cum_t[:, h : h + 1] - cum[h : h + 1, :], -1e30))
            hi, lo = split2(decay * scores * step[h : h + 1, :])
            halves.append(mm(hi, x, 1, 0) + mm(lo, x, 1, 0))
        skip = jnp.where(first[:1], skip_ref[2 * pair], skip_ref[2 * pair + 1])
        mixed = jnp.where(first, halves[0], halves[1]) + skip * x.astype(F32)
        mixed_ref[:, at] = mixed
        gate = gate_ref[:, at].astype(F32)
        gated = mixed * gate * jax.nn.sigmoid(gate)
        gated_ref[:, at] = gated
        square = square + jnp.sum(gated * gated, axis=1, keepdims=True)
    inverse = lax.rsqrt(square * (1.0 / D) + 1e-05)
    for k in range(8):
        at = slice(k * 128, (k + 1) * 128)
        normed = (gated_ref[:, at] * inverse * gain_ref[:, at]).astype(BF)
        for x_b in range(2):
            out_ref[k % 2 * 2 + x_b, :, k // 2 * 128 : k // 2 * 128 + 128] = normed


def forward_call(dl, sb, skip, x, gate, b, c, raw, gain):
    return pl.pallas_call(
        forward_kernel,
        out_shape=(jax.ShapeDtypeStruct((L, D), F32), jax.ShapeDtypeStruct((4, L, D // 2), BF)),
        in_specs=[SM] * 3 + [VM] * 6,
        out_specs=(VM, VM),
        scratch_shapes=[pltpu.VMEM((L, D), F32)],
        cost_estimate=pl.CostEstimate(flops=3 * 10**9, bytes_accessed=3 * 10**6, transcendentals=10**6),
        name="mix_forward",
    )(dl, sb, skip, x, gate, b, c, raw, gain)


def backward_kernel(
    place_ref, dl_ref, sb_ref, skip_ref, x_ref, gate_ref, b_ref, c_ref, raw_ref, gain_ref, mixed_ref, *refs,
):
    part0, part1, part2, part3, *refs = refs
    backward_body(place_ref[1] < 2, dl_ref, sb_ref, skip_ref, x_ref, gate_ref, b_ref, c_ref, raw_ref, gain_ref, mixed_ref, (part0, part1), (part2, part3), *refs)


def backward_body(
    low, dl_ref, sb_ref, skip_ref, x_ref, gate_ref, b_ref, c_ref, raw_ref, gain_ref, mixed_ref, own_refs, other_refs,
    dx_ref, dgate_ref, db_ref, dc_ref, draw_ref, scal_ref, dgain_ref,
    gn_ref, gated_ref, dm_ref, row_ref, dir_ref,
):
    square = jnp.zeros((L, 1), F32)
    inner = jnp.zeros((L, 1), F32)
    for k in range(8):
        at = slice(k * 128, (k + 1) * 128)
        within = slice(k // 2 * 128, k // 2 * 128 + 128)
        own, other = (a[:, within].astype(F32) + b[:, within].astype(F32) for a, b in (own_refs, other_refs))
        gn = jnp.where(low, own, other) if k % 2 == 0 else jnp.where(low, other, own)
        gn_ref[:, at] = gn
        gate = gate_ref[:, at].astype(F32)
        gated = mixed_ref[:, at] * gate * jax.nn.sigmoid(gate)
        gated_ref[:, at] = gated
        square = square + jnp.sum(gated * gated, axis=1, keepdims=True)
        inner = inner + jnp.sum(gn * gain_ref[:, at] * gated, axis=1, keepdims=True)
    inverse = lax.rsqrt(square * (1.0 / D) + 1e-05)
    back = inner * inverse * inverse * (1.0 / D)
    for k in range(8):
        at = slice(k * 128, (k + 1) * 128)
        gated, gn = gated_ref[:, at], gn_ref[:, at]
        dgain_ref[:, at] = jnp.sum(gn * gated * inverse, axis=0, keepdims=True)
        dgated = inverse * (gn * gain_ref[:, at] - gated * back)
        gate = gate_ref[:, at].astype(F32)
        sig = jax.nn.sigmoid(gate)
        dm_ref[:, at] = dgated * gate * sig
        dgate_ref[:, at] = (dgated * mixed_ref[:, at] * sig * (1.0 + gate * (1.0 - sig))).astype(BF)

    step_bias = column(sb_ref)
    step, rate, cum = steps_and_decay(raw_ref[...], column(dl_ref), step_bias)
    cum_t = cum.T
    scores = mm(c_ref[...], b_ref[...], 1, 1)
    causal = causal_mask()
    first = lax.broadcasted_iota(jnp.int32, (L, 2 * PS), 1) < PS
    head_of = lax.broadcasted_iota(jnp.int32, (L, H), 1)
    dscores = jnp.zeros((L, L), F32)
    rows = jnp.zeros((L, H), F32)
    for pair in range(H // 2):
        at = slice(pair * 128, (pair + 1) * 128)
        x = x_ref[:, at]
        dm = dm_ref[:, at]
        dm_hi, dm_lo = split2(dm)
        dx_halves = []
        for k in range(2):
            h = 2 * pair + k
            mine = first if k == 0 else jnp.logical_not(first)
            decay = jnp.exp(jnp.where(causal, cum_t[:, h : h + 1] - cum[h : h + 1, :], -1e30))
            kernel = decay * scores
            hi, lo = split2(kernel * step[h : h + 1, :])
            dx_halves.append(mm(hi, dm_hi, 0, 0) + mm(lo, dm_hi, 0, 0) + mm(hi, dm_lo, 0, 0))
            x_mine = jnp.where(mine, x, jnp.zeros_like(x))
            dweights = mm(dm_hi, x_mine, 1, 1) + mm(dm_lo, x_mine, 1, 1)
            direct = dweights * kernel
            dir_ref[h : h + 1, :] = jnp.sum(direct, axis=0, keepdims=True)
            rows = jnp.where(head_of == h, jnp.sum(direct * step[h : h + 1, :], axis=1, keepdims=True), rows)
            dscores = dscores + dweights * decay * step[h : h + 1, :]
        skip = jnp.where(first[:1], skip_ref[2 * pair], skip_ref[2 * pair + 1])
        dx_ref[:, at] = (jnp.where(first, dx_halves[0], dx_halves[1]) + skip * dm).astype(BF)
        row_ref[:, at] = jnp.sum(dm * x.astype(F32), axis=0, keepdims=True)
    d_hi, d_lo = split2(dscores)
    dc_ref[...] = (mm(d_hi, b_ref[...], 1, 0) + mm(d_lo, b_ref[...], 1, 0)).astype(BF)
    db_ref[...] = (mm(d_hi, c_ref[...], 0, 0) + mm(d_lo, c_ref[...], 0, 0)).astype(BF)
    direct = dir_ref[...]
    dcum = rows.T - direct * step
    t = lax.broadcasted_iota(jnp.int32, (L, L), 0)
    s = lax.broadcasted_iota(jnp.int32, (L, L), 1)
    onward = (t >= s).astype(BF)
    dsum = sum(mm(part, onward, 1, 0) for part in split3(dcum))
    dstep = direct + dsum * rate
    draw = dstep * jax.nn.sigmoid(raw_ref[...] + step_bias)
    draw_ref[...] = draw
    lane = lax.broadcasted_iota(jnp.int32, (H, 128), 1)
    ddecay = jnp.sum(dsum * step, axis=1, keepdims=True) * rate
    dbias = jnp.sum(draw, axis=1, keepdims=True)
    chan = lax.broadcasted_iota(jnp.int32, (H, D), 1) // PS
    head = lax.broadcasted_iota(jnp.int32, (H, D), 0)
    dskip = jnp.sum(jnp.where(chan == head, row_ref[...], 0.0), axis=1, keepdims=True)
    scal_ref[...] = jnp.where(lane == 0, ddecay, jnp.where(lane == 1, dbias, jnp.where(lane == 2, dskip, 0.0)))


def backward_call(place, dl, sb, skip, x, gate, b, c, raw, gain, mixed, *parts):
    sds = jax.ShapeDtypeStruct
    return pl.pallas_call(
        backward_kernel,
        out_shape=(
            sds((L, D), BF), sds((L, D), BF), sds((L, N), BF), sds((L, N), BF), sds((H, L), F32), sds((H, 128), F32), sds((1, D), F32),
        ),
        in_specs=[SM] * 4 + [VM] * 11,
        out_specs=(VM,) * 7,
        scratch_shapes=[pltpu.VMEM((L, D), F32)] * 3 + [pltpu.VMEM((1, D), F32), pltpu.VMEM((H, L), F32)],
        cost_estimate=pl.CostEstimate(flops=6 * 10**9, bytes_accessed=5 * 10**6, transcendentals=10**6),
        name="mix_backward",
    )(place, dl, sb, skip, x, gate, b, c, raw, gain, mixed, *parts)


def spread_kernel(place_ref, og0, og1, og2, og3, own_ref, other_ref, out0, out1, out2, out3, w_ref):
    core = place_ref[0]
    for r in range(8):
        at = pl.multiple_of(64 * r + 32 * core, 32)
        w_ref[pl.ds(at, 32), :] = own_ref[32 * r : 32 * r + 32, :]
        at = pl.multiple_of(64 * r + 32 * (1 - core), 32)
        w_ref[pl.ds(at, 32), :] = other_ref[32 * r : 32 * r + 32, :]
    for ref, out in zip((og1, og3, og2, og0), (out1, out3, out2, out0)):
        out[...] = mm(ref[...], w_ref[...], 1, 1).astype(BF)


def spread_call(place, og, own, other):
    half = own.shape[1]
    return pl.pallas_call(
        spread_kernel,
        out_shape=(jax.ShapeDtypeStruct((L, D // 2), BF),) * 4,
        in_specs=[SM] + [VM] * 6,
        out_specs=(VM,) * 4,
        scratch_shapes=[pltpu.VMEM((D // 2, half), BF)],
        cost_estimate=pl.CostEstimate(flops=4 * L * half * D, bytes_accessed=4 * 10**6, transcendentals=0),
        name="node_spread",
    )(place, *og, own, other)


def term_kernel(place_ref, normed_ref, og0, og1, og2, og3, keep_ref, send_ref, acc_ref):
    core, chip = place_ref[0], place_ref[1]
    for k, ref in enumerate((og0, og1, og2, og3)):
        add = mm(normed_ref[jnp.bitwise_xor(chip, k)], ref[...], 0, 0)
        acc_ref[...] = add if k == 0 else acc_ref[...] + add
    for r in range(8):
        at = pl.multiple_of(64 * r + 32 * core, 32)
        keep_ref[32 * r : 32 * r + 32, :] = acc_ref[pl.ds(at, 32), :].astype(BF)
        at = pl.multiple_of(64 * r + 32 * (1 - core), 32)
        send_ref[32 * r : 32 * r + 32, :] = acc_ref[pl.ds(at, 32), :].astype(BF)


def term_call(place, normed, og):
    half = og[0].shape[1]
    out = jax.ShapeDtypeStruct((D // 4, half), BF)
    return pl.pallas_call(
        term_kernel,
        out_shape=(out, out),
        in_specs=[SM] + [VM] * 5,
        out_specs=(VM, VM),
        scratch_shapes=[pltpu.VMEM((D // 2, half), F32)],
        cost_estimate=pl.CostEstimate(flops=4 * L * half * D, bytes_accessed=4 * 10**6, transcendentals=0),
        name="node_term",
    )(place, normed, *og)


def part_of(value, index):
    return lax.dynamic_index_in_dim(value, index, 0, keepdims=False)


def in_order(parts, first):
    count = len(parts)
    return lax.dynamic_slice_in_dim(jnp.stack(parts * 2), (count - first) % count, count, 0)


def shards(
    scan_input,
    gate_input,
    write_proj,
    read_proj,
    step_raw,
    decay_log,
    step_bias,
    skip_gain,
    norm_gain,
    out_weight,
    out_grad,
):
    tokens, cols = out_grad.shape
    own_rows = out_weight.shape[0]
    half, third = cols // 2, cols // 6
    x_a, x_b, core, z_lo = (lax.axis_index(n) for n in ("xa", "xb", "c", "zl"))
    place = jnp.stack([core, 2 * x_a + x_b]).astype(jnp.int32)

    def exchanged(tiles, axes):
        return lax.all_to_all(tiles, axes, 0, 0, tiled=True)

    tiles = out_weight.reshape(own_rows, 2, 3, third)
    tiles = lax.dynamic_index_in_dim(tiles, z_lo, 2, keepdims=False).transpose(1, 0, 2)
    tiles = jnp.broadcast_to(tiles[None], (4, 2, own_rows, third)).reshape(8, own_rows, third)
    line = exchanged(tiles, ("zh", "xb")).reshape(8 * own_rows, third)
    w_next = lax.ppermute(line, LINE, along_line(-1))
    w_last = lax.ppermute(line, LINE, along_line(1))
    w_own = in_order([line, w_next, w_last], z_lo).transpose(1, 0, 2).reshape(8 * own_rows, half)
    w_other = lax.ppermute(w_own, "c", SWAP)

    halves = out_grad.reshape(tokens, 2, half).transpose(1, 0, 2)
    kept, sent = part_of(halves, x_b), part_of(halves, 1 - x_b)
    og = [
        kept,
        lax.ppermute(sent, "xb", SWAP),
        lax.ppermute(kept, "xa", SWAP),
        lax.ppermute(sent, NODE, [(i, 3 - i) for i in range(4)]),
    ]

    small = (decay_log, step_bias, skip_gain)
    large = (scan_input, gate_input, write_proj, read_proj, step_raw, norm_gain[None])
    mixed, normed = forward_call(*small, *large)
    normed_node = exchanged(normed, NODE)
    partial = spread_call(place, og, w_own, w_other)
    partial = [
        partial[0],
        lax.ppermute(partial[1], "xb", SWAP),
        lax.ppermute(partial[2], "xa", SWAP),
        lax.ppermute(partial[3], NODE, [(i, 3 - i) for i in range(4)]),
    ]
    *gradients, scalars, grad_gain = backward_call(place, *small, *large, mixed, *partial)

    keep, send = term_call(place, normed_node, og)
    term = keep.astype(F32) + lax.ppermute(send, "c", SWAP).astype(F32)
    rows = own_rows // 8
    term = term.astype(BF).reshape(8, 8, rows, 3, third).transpose(1, 3, 0, 2, 4)
    pieces = exchanged(term.reshape(24, 8 * rows, third), ("y", "zl"))
    piece = pieces.astype(F32).sum(0).astype(BF).reshape(8, 3 * rows, 128)

    totals = jnp.concatenate([grad_gain[0], scalars[:, :8].reshape(-1)]).reshape(9, 128)
    for axes in ("c", "xa"):
        totals = lax.psum(totals, axes)
    both = jnp.concatenate(split2(totals))
    piece = jnp.concatenate([piece, jnp.broadcast_to(both[None], (8, *both.shape))], axis=1)
    piece = exchanged(piece, ("zh", "xb")).astype(F32)
    totals = piece[:, 3 * rows :].sum(0)
    totals = totals[:9] + totals[9:]
    piece = piece[:, : 3 * rows].reshape(4, 2, 3 * rows, 128).sum(0)
    owned = jnp.concatenate([piece.astype(BF).reshape(-1, 128), *split2(totals)])
    owned = exchanged(jnp.broadcast_to(owned[None], (24, *owned.shape)), ("y", "zl"))
    blocks = owned[:, : 6 * rows].reshape(8, 3, 2, rows, third).transpose(0, 3, 2, 1, 4)
    grad_weight = blocks.astype(F32).reshape(own_rows, cols)
    totals = owned[:, 6 * rows :].astype(F32).reshape(24, 2, 9 * 128).sum((0, 1))
    small_totals = totals[D:].reshape(H, 8)
    return (grad_weight, *gradients, small_totals[:, 0], small_totals[:, 1], small_totals[:, 2], totals[:D])


def solution(mesh):
    torus = Mesh(mesh.devices.reshape(8, 3, 4, 2, 2, 2), AXES)
    split, whole = P(AXES, None), P()
    return jax.shard_map(
        shards,
        mesh=torus,
        in_specs=(split,) * 4 + (P(None, AXES),) + (whole,) * 4 + (P(REPLICA, None), split),
        out_specs=(P(REPLICA, None),) + (split,) * 4 + (P(None, AXES),) + (whole,) * 4,
        check_vma=False,
    )
```
